32 devices in a mesh: clips: 1, frame: 32 (over z, y, x, core).
Axes of the slice: x: 2, y: 2, z: 4, core: 2. Of those that a mesh axis runs over, the one named last changes fastest.
Arguments:
- frame_sequence_elements: bfloat16 [32, 256, 1280], P(('clips', 'frame')), may hold values from -8 to 8
- entry_rescaling_factors: float32 [1280], replicated, may hold values from 0.5 to 1.5
- asking_projection_tensor: bfloat16 [1280, 640], replicated, may hold values from -1 to 1
- lookup_projection_tensor: bfloat16 [1280, 640], replicated, may hold values from -1 to 1
- content_projection_tensor: bfloat16 [1280, 640], replicated, may hold values from -0.15625 to 0.15625
- logit_sharpness: float32 [5], replicated, may hold values from 0.3 to 24
- final_projection_tensor: bfloat16 [640, 1280], replicated, may hold values from -0.25 to 0.25
Outputs:
- mixed: bfloat16 [32, 256, 1280], P(('clips', 'frame'))
The draws below stay inside these ranges and needn't reach their ends.
All inputs are finite; a program needn't handle non-finite values.
Results may differ from the reference program's by a relative error of at most 0.006.
Values may be sent and summed in bfloat16 or wider, within the bound.
A program may use at most 64 MiB of HBM per device.

```python
import math
import jax
import jax.numpy as jnp
from jax import lax

D = 1280
HEADS_WIN = 5
CHANNELS_PER_ATT = 128
S = 256
WINDOW = 32
QW = 640
FRAMES = 32


def draw_frame_sequence_elements(key, part):
    values = jax.random.normal(jax.random.fold_in(key, 1), (FRAMES, S, D), jnp.float32)
    return jnp.clip(values, -8.0, 8.0).astype(jnp.bfloat16)


def shared_rows(key):
    return jnp.clip(jax.random.normal(jax.random.fold_in(key, 7), (D, QW), jnp.float32), -6.0, 6.0)


def draw_asking_projection_tensor(key, part):
    return (shared_rows(key) / math.sqrt(D)).astype(jnp.bfloat16)


def draw_lookup_projection_tensor(key, part):
    jitter = jnp.clip(jax.random.normal(jax.random.fold_in(key, 13), (D, QW), jnp.float32), -6.0, 6.0)
    values = jitter / math.sqrt(D)
    return values.astype(jnp.bfloat16)


def draw_logit_sharpness(key, part):
    lower, upper = (0.3, 3.0)
    level = jax.random.uniform(jax.random.fold_in(key, 17), (HEADS_WIN,), jnp.float32, math.log(lower), math.log(upper))
    return jnp.exp(level)


def centred(own_key, extent, width, reach, kind=jnp.bfloat16):
    return jnp.clip(width * jax.random.normal(own_key, extent, jnp.float32), -reach, reach).astype(kind)


def setup_inputs(seed: int = 0, part: int = 0) -> dict:
    splits = jax.random.split(jax.random.key(seed), 8)
    part_keys = jax.random.split(jax.random.fold_in(splits[7], part), 8)
    frame_sequence_elements = draw_frame_sequence_elements(jax.random.fold_in(jax.random.fold_in(splits[7], part), 71), part)
    entry_rescaling_factors = jnp.clip(1.0 + 0.1 * jax.random.normal(splits[1], (D,), jnp.float32), 0.5, 1.5)
    asking_projection_tensor = draw_asking_projection_tensor(jax.random.fold_in(splits[7], 71), part)
    lookup_projection_tensor = draw_lookup_projection_tensor(jax.random.fold_in(splits[7], 71), part)
    content_projection_tensor = centred(splits[4], (D, QW), D ** -0.5, 0.15625)
    logit_sharpness = draw_logit_sharpness(jax.random.fold_in(splits[7], 71), part)
    final_projection_tensor = centred(splits[6], (QW, D), QW ** -0.5, 0.25)
    return dict(frame_sequence_elements=frame_sequence_elements, entry_rescaling_factors=entry_rescaling_factors, asking_projection_tensor=asking_projection_tensor, lookup_projection_tensor=lookup_projection_tensor, content_projection_tensor=content_projection_tensor, logit_sharpness=logit_sharpness, final_projection_tensor=final_projection_tensor)


epsilon = 1e-06

def quadratic_average_rescaling(values):
    return values * lax.rsqrt(lax.optimization_barrier(jnp.mean(values * values, axis=-1, keepdims=True)) + epsilon)

def reference(frame_sequence_elements, entry_rescaling_factors, asking_projection_tensor, lookup_projection_tensor, content_projection_tensor, logit_sharpness, final_projection_tensor):
    floated = frame_sequence_elements.astype(jnp.float32)
    rescaled_token_vectors = (quadratic_average_rescaling(floated) * entry_rescaling_factors).astype(jnp.bfloat16)
    flat_rows = rescaled_token_vectors.reshape(FRAMES * S, D)
    shape_heads = (FRAMES, S, HEADS_WIN, CHANNELS_PER_ATT)
    asking_vectors_full = jnp.dot(flat_rows, asking_projection_tensor, preferred_element_type=jnp.float32).reshape(shape_heads)
    k_full = jnp.dot(flat_rows, lookup_projection_tensor, preferred_element_type=jnp.float32).reshape(shape_heads)
    v_full = jnp.dot(flat_rows, content_projection_tensor, preferred_element_type=jnp.float32).reshape(shape_heads)
    asking_token_vectors = (quadratic_average_rescaling(asking_vectors_full) * logit_sharpness[:, None] / math.sqrt(CHANNELS_PER_ATT)).astype(jnp.bfloat16)
    key_matrix_rows = quadratic_average_rescaling(k_full).astype(jnp.bfloat16)
    value_matrix_rows = v_full.astype(jnp.bfloat16)
    frame_ids = jnp.arange(FRAMES, dtype=jnp.int32)
    offset = frame_ids[:, None] - frame_ids[None, :]
    window_mask = (offset >= 0) & (offset < WINDOW)

    def column(pieces):
        q_col, k_col, v_col = pieces
        scores = jnp.einsum('thd,shd->hts', q_col.astype(jnp.float32), k_col.astype(jnp.float32))
        scores = jnp.where(window_mask[None], scores, -1e+30)
        top = lax.optimization_barrier(jnp.max(scores, axis=-1, keepdims=True))
        expo = jnp.exp(scores - top)
        weights = (expo / lax.optimization_barrier(jnp.sum(expo, axis=-1, keepdims=True))).astype(jnp.bfloat16)
        attended = jnp.einsum('hts,shd->thd', weights.astype(jnp.float32), v_col.astype(jnp.float32))
        return attended.astype(jnp.bfloat16)
    per_column = lax.map(column, (asking_token_vectors.transpose(1, 0, 2, 3), key_matrix_rows.transpose(1, 0, 2, 3), value_matrix_rows.transpose(1, 0, 2, 3)))
    attended = per_column.transpose(1, 0, 2, 3).reshape(FRAMES * S, QW)
    summed = jnp.dot(attended, final_projection_tensor, preferred_element_type=jnp.float32) + floated.reshape(FRAMES * S, D)
    return summed.astype(jnp.bfloat16).reshape(FRAMES, S, D)
```

```python
import functools
import math

import jax
import jax.numpy as jnp
from jax import lax
from jax.experimental import pallas as pl
from jax.experimental.pallas import tpu as pltpu
from jax.sharding import PartitionSpec as P

HEADS_WIN = 5
CHANNELS_PER_ATT = 128
WINDOW = 32


epsilon = 1e-06


def quadratic_average_rescaling(values):
    return values * lax.rsqrt(jnp.mean(values * values, axis=-1, keepdims=True) + epsilon)


def project_through(
    incoming_token_vectors,
    asking_projection_tensor,
    lookup_projection_tensor,
    content_projection_tensor,
    logit_sharpness,
):
    lead = incoming_token_vectors.shape[:-1]
    flat_rows = incoming_token_vectors.reshape(-1, incoming_token_vectors.shape[-1])
    shape_heads = lead + (HEADS_WIN, CHANNELS_PER_ATT)
    asking_vectors_full = jnp.dot(
        flat_rows, asking_projection_tensor, preferred_element_type=jnp.float32
    ).reshape(shape_heads)
    k_full = jnp.dot(
        flat_rows, lookup_projection_tensor, preferred_element_type=jnp.float32
    ).reshape(shape_heads)
    v_full = jnp.dot(
        flat_rows, content_projection_tensor, preferred_element_type=jnp.float32
    ).reshape(shape_heads)
    asking_token_vectors = (
        quadratic_average_rescaling(asking_vectors_full)
        * logit_sharpness[:, None]
        / math.sqrt(CHANNELS_PER_ATT)
    ).astype(jnp.bfloat16)
    key_matrix_rows = quadratic_average_rescaling(k_full).astype(jnp.bfloat16)
    return (asking_token_vectors, key_matrix_rows, v_full.astype(jnp.bfloat16))


def softmax_bf16(scores, window_mask):
    scores = jnp.where(window_mask, scores, -1e30)
    top = jnp.max(scores, axis=-1, keepdims=True)
    expo = jnp.exp(scores - top)
    return (expo / jnp.sum(expo, axis=-1, keepdims=True)).astype(jnp.bfloat16)


def band_attention(asking_token_vectors, key_matrix_rows, value_matrix_rows):
    all_frames, positions, heads, width = asking_token_vectors.shape
    blocks = all_frames // WINDOW
    block_shape = (blocks, WINDOW, positions, heads, width)
    q_blocks = asking_token_vectors.reshape(block_shape)
    k_blocks = key_matrix_rows.reshape(block_shape)
    v_blocks = value_matrix_rows.reshape(block_shape)
    k_earlier = jnp.concatenate([jnp.zeros_like(k_blocks[:1]), k_blocks[:-1]], axis=0)
    v_earlier = jnp.concatenate([jnp.zeros_like(v_blocks[:1]), v_blocks[:-1]], axis=0)
    k_pair = jnp.concatenate([k_earlier, k_blocks], axis=1)
    v_pair = jnp.concatenate([v_earlier, v_blocks], axis=1)
    scores = jnp.einsum("bqphd,bkphd->bphqk", q_blocks, k_pair, preferred_element_type=jnp.float32)
    block_ids = jnp.arange(blocks, dtype=jnp.int32)[:, None, None]
    row_ids = jnp.arange(WINDOW, dtype=jnp.int32)[None, :, None]
    col_ids = jnp.arange(2 * WINDOW, dtype=jnp.int32)[None, None, :]
    offset = row_ids - col_ids + WINDOW
    inside = (offset >= 0) & (offset < WINDOW) & (block_ids * WINDOW - WINDOW + col_ids >= 0)
    weights = softmax_bf16(scores, inside[:, None, None])
    attended = jnp.einsum("bphqk,bkphd->bqphd", weights, v_pair, preferred_element_type=jnp.float32)
    return attended.astype(jnp.bfloat16).reshape(all_frames, positions, heads, width)


def local(
    frame_sequence_elements,
    entry_rescaling_factors,
    asking_projection_tensor,
    lookup_projection_tensor,
    content_projection_tensor,
    logit_sharpness,
    final_projection_tensor,
):
    frames_dev, seq_len, width = frame_sequence_elements.shape
    floated = frame_sequence_elements.astype(jnp.float32)
    rescaled_token_vectors = (
        quadratic_average_rescaling(floated) * entry_rescaling_factors
    ).astype(jnp.bfloat16)
    position_rows = lax.all_to_all(
        rescaled_token_vectors, "frame", split_axis=1, concat_axis=0, tiled=True
    )
    asking_token_vectors, key_matrix_rows, value_matrix_rows = project_through(
        position_rows,
        asking_projection_tensor,
        lookup_projection_tensor,
        content_projection_tensor,
        logit_sharpness,
    )
    result = band_attention(asking_token_vectors, key_matrix_rows, value_matrix_rows)
    attended = lax.all_to_all(result, "frame", split_axis=0, concat_axis=1, tiled=True)
    flat_attended = attended.reshape(frames_dev * seq_len, -1)
    summed = jnp.dot(
        flat_attended, final_projection_tensor, preferred_element_type=jnp.float32
    ) + floated.reshape(frames_dev * seq_len, width)
    return summed.astype(jnp.bfloat16).reshape(frames_dev, seq_len, width)


MESH = pl.DeviceIdType.MESH
HIGH = HEADS_WIN * CHANNELS_PER_ATT


def visiting_order(devices):
    return sorted(range(1, devices), key=lambda k: (abs(k - devices // 2), k))


def fused(
    devices,
    local_frames,
    sharp_ref,
    x_hbm,
    gain_ref,
    wq_hbm,
    wk_hbm,
    wv_hbm,
    wo_hbm,
    out_ref,
    x_own,
    wq,
    wk,
    wv,
    wo,
    gathered,
    q_rows,
    k_rows,
    v_rows,
    outgoing,
    returned,
    load_sem,
    send_a,
    recv_a,
    send_b,
    recv_b,
):
    me = lax.axis_index("frame")
    block, width = x_own.shape[1], x_own.shape[2]
    positions = block // local_frames
    order = visiting_order(devices)

    barrier = pltpu.get_barrier_semaphore()
    for k in order:
        pl.semaphore_signal(
            barrier, inc=1, device_id={"frame": lax.rem(me + k, devices)}, device_id_type=MESH
        )
    loads = [
        pltpu.make_async_copy(source, target, load_sem.at[i])
        for i, (source, target) in enumerate(
            ((x_hbm, x_own), (wq_hbm, wq), (wk_hbm, wk), (wv_hbm, wv), (wo_hbm, wo))
        )
    ]
    for load in loads:
        load.start()
    loads[0].wait()
    pl.semaphore_wait(barrier, devices - 1)

    first = {}
    for k in order:
        target = lax.rem(me + k, devices)
        first[k] = pltpu.make_async_remote_copy(
            src_ref=x_own.at[target],
            dst_ref=gathered.at[k],
            send_sem=send_a.at[k],
            recv_sem=recv_a.at[k],
            device_id={"frame": target},
            device_id_type=MESH,
        )
        first[k].start()
    gathered[0] = x_own[me]
    for load in loads[1:]:
        load.wait()

    def project(start, stop):
        rows = (stop - start) * block
        at = slice(start * block, stop * block)
        x = gathered[start:stop].astype(jnp.float32).reshape(rows, width)
        normed = (quadratic_average_rescaling(x) * gain_ref[...]).astype(jnp.bfloat16)
        q = jnp.dot(normed, wq[...], preferred_element_type=jnp.float32)
        k = jnp.dot(normed, wk[...], preferred_element_type=jnp.float32)
        v = jnp.dot(normed, wv[...], preferred_element_type=jnp.float32)
        for h in range(HEADS_WIN):
            c = slice(h * CHANNELS_PER_ATT, (h + 1) * CHANNELS_PER_ATT)
            q_rows[at, c] = (
                quadratic_average_rescaling(q[:, c]) * sharp_ref[h] / math.sqrt(CHANNELS_PER_ATT)
            ).astype(jnp.bfloat16)
            k_rows[at, c] = quadratic_average_rescaling(k[:, c]).astype(jnp.bfloat16)
        v_rows[at, :] = v.astype(jnp.bfloat16)

    quarter = devices // 4
    pieces = ((quarter, devices - quarter), (devices - quarter, devices), (0, quarter))
    for start, stop in pieces:
        for k in range(max(start, 1), stop):
            first[k].wait_recv()
        project(start, stop)

    total = devices * block
    def ids(axis):
        r = lax.broadcasted_iota(jnp.int32, (total, total), axis)
        slot = r // block
        owner = me - slot
        owner = jnp.where(owner < 0, owner + devices, owner)
        inner = r - slot * block
        return owner * local_frames + inner // positions, inner % positions

    t_row, p_row = ids(0)
    t_col, p_col = ids(1)
    offset = t_row - t_col
    inside = (p_row == p_col) & (offset >= 0) & (offset < WINDOW)
    for h in range(HEADS_WIN):
        c = slice(h * CHANNELS_PER_ATT, (h + 1) * CHANNELS_PER_ATT)
        scores = lax.dot_general(
            q_rows[:, c], k_rows[:, c], (((1,), (1,)), ((), ())), preferred_element_type=jnp.float32
        )
        weights = softmax_bf16(scores, inside)
        attended = jnp.dot(weights, v_rows[:, c], preferred_element_type=jnp.float32)
        outgoing[:, :, c] = attended.reshape(devices, block, CHANNELS_PER_ATT).astype(jnp.bfloat16)

    second = {}
    for k in order:
        target = lax.rem(me + devices - k, devices)
        second[k] = pltpu.make_async_remote_copy(
            src_ref=outgoing.at[k],
            dst_ref=returned.at[me],
            send_sem=send_b.at[k],
            recv_sem=recv_b.at[k],
            device_id={"frame": target},
            device_id_type=MESH,
        )
        second[k].start()
    returned[me] = outgoing[0]
    for k in order:
        pltpu.make_async_remote_copy(
            src_ref=outgoing.at[k],
            dst_ref=returned.at[lax.rem(me + k, devices)],
            send_sem=send_b.at[k],
            recv_sem=recv_b.at[k],
            device_id={"frame": lax.rem(me + devices - k, devices)},
            device_id_type=MESH,
        ).wait_recv()
    mixed = returned[...].astype(jnp.float32).reshape(total, HIGH).astype(jnp.bfloat16)
    summed = jnp.dot(mixed, wo[...], preferred_element_type=jnp.float32)
    summed = summed + x_own[...].astype(jnp.float32).reshape(total, width)
    out_ref[...] = summed.reshape(devices, block, width).astype(jnp.bfloat16)
    for k in order:
        first[k].wait_send()
        second[k].wait_send()


def local_fused(devices, x, gain, wq, wk, wv, sharp, wo):
    local_frames, seq_len, width = x.shape
    positions = seq_len // devices
    block = local_frames * positions
    total = devices * block
    blocks = x.reshape(local_frames, devices, positions, width)
    blocks = blocks.transpose(1, 0, 2, 3).reshape(devices, block, width)
    vmem = pl.BlockSpec(memory_space=pltpu.VMEM)
    anywhere = pl.BlockSpec(memory_space=pl.ANY)
    dma = pltpu.SemaphoreType.DMA
    out = pl.pallas_call(
        functools.partial(fused, devices, local_frames),
        out_shape=jax.ShapeDtypeStruct(blocks.shape, jnp.bfloat16),
        in_specs=[pl.BlockSpec(memory_space=pltpu.SMEM), anywhere, vmem] + [anywhere] * 4,
        out_specs=vmem,
        scratch_shapes=[
            pltpu.VMEM(blocks.shape, jnp.bfloat16),
            pltpu.VMEM(wq.shape, jnp.bfloat16),
            pltpu.VMEM(wk.shape, jnp.bfloat16),
            pltpu.VMEM(wv.shape, jnp.bfloat16),
            pltpu.VMEM(wo.shape, jnp.bfloat16),
            pltpu.VMEM(blocks.shape, jnp.bfloat16),
            pltpu.VMEM((total, HIGH), jnp.bfloat16),
            pltpu.VMEM((total, HIGH), jnp.bfloat16),
            pltpu.VMEM((total, HIGH), jnp.bfloat16),
            pltpu.VMEM((devices, block, HIGH), jnp.bfloat16),
            pltpu.VMEM((devices, block, HIGH), jnp.bfloat16),
            dma((5,)),
            dma((devices,)),
            dma((devices,)),
            dma((devices,)),
            dma((devices,)),
        ],
        compiler_params=pltpu.CompilerParams(
            collective_id=0, has_side_effects=True, vmem_limit_bytes=60 * 2**20
        ),
    )(sharp, blocks, gain.reshape(1, width), wq, wk, wv, wo)
    out = out.reshape(devices, local_frames, positions, width).transpose(1, 0, 2, 3)
    return out.reshape(x.shape)


def solution(mesh):
    devices = mesh.shape["frame"]

    def body(x, *rest):
        positions = x.shape[1] // devices
        if devices % 4 == 0 and positions % 8 == 0:
            return local_fused(devices, x, *rest)
        return local(x, *rest)

    placed = (P(("clips", "frame"), None, None), P(), P(), P(), P(), P(), P())
    return jax.shard_map(
        body,
        mesh=mesh,
        in_specs=placed,
        out_specs=P(("clips", "frame"), None, None),
        check_vma=False,
    )
```

```python
import functools
import math

import jax
import jax.numpy as jnp
from jax import lax
from jax.experimental import pallas as pl
from jax.experimental.pallas import tpu as pltpu
from jax.sharding import PartitionSpec as P

HEADS_WIN = 5
CHANNELS_PER_ATT = 128
WINDOW = 32


epsilon = 1e-06


def quadratic_average_rescaling(values):
    return values * lax.rsqrt(jnp.mean(values * values, axis=-1, keepdims=True) + epsilon)


def project_through(
    incoming_token_vectors,
    asking_projection_tensor,
    lookup_projection_tensor,
    content_projection_tensor,
    logit_sharpness,
):
    lead = incoming_token_vectors.shape[:-1]
    flat_rows = incoming_token_vectors.reshape(-1, incoming_token_vectors.shape[-1])
    shape_heads = lead + (HEADS_WIN, CHANNELS_PER_ATT)
    asking_vectors_full = jnp.dot(
        flat_rows, asking_projection_tensor, preferred_element_type=jnp.float32
    ).reshape(shape_heads)
    k_full = jnp.dot(
        flat_rows, lookup_projection_tensor, preferred_element_type=jnp.float32
    ).reshape(shape_heads)
    v_full = jnp.dot(
        flat_rows, content_projection_tensor, preferred_element_type=jnp.float32
    ).reshape(shape_heads)
    asking_token_vectors = (
        quadratic_average_rescaling(asking_vectors_full)
        * logit_sharpness[:, None]
        / math.sqrt(CHANNELS_PER_ATT)
    ).astype(jnp.bfloat16)
    key_matrix_rows = quadratic_average_rescaling(k_full).astype(jnp.bfloat16)
    return (asking_token_vectors, key_matrix_rows, v_full.astype(jnp.bfloat16))


def softmax_bf16(scores, window_mask):
    scores = jnp.where(window_mask, scores, -1e30)
    top = jnp.max(scores, axis=-1, keepdims=True)
    expo = jnp.exp(scores - top)
    return (expo / jnp.sum(expo, axis=-1, keepdims=True)).astype(jnp.bfloat16)


def band_attention(asking_token_vectors, key_matrix_rows, value_matrix_rows):
    all_frames, positions, heads, width = asking_token_vectors.shape
    blocks = all_frames // WINDOW
    block_shape = (blocks, WINDOW, positions, heads, width)
    q_blocks = asking_token_vectors.reshape(block_shape)
    k_blocks = key_matrix_rows.reshape(block_shape)
    v_blocks = value_matrix_rows.reshape(block_shape)
    k_earlier = jnp.concatenate([jnp.zeros_like(k_blocks[:1]), k_blocks[:-1]], axis=0)
    v_earlier = jnp.concatenate([jnp.zeros_like(v_blocks[:1]), v_blocks[:-1]], axis=0)
    k_pair = jnp.concatenate([k_earlier, k_blocks], axis=1)
    v_pair = jnp.concatenate([v_earlier, v_blocks], axis=1)
    scores = jnp.einsum("bqphd,bkphd->bphqk", q_blocks, k_pair, preferred_element_type=jnp.float32)
    block_ids = jnp.arange(blocks, dtype=jnp.int32)[:, None, None]
    row_ids = jnp.arange(WINDOW, dtype=jnp.int32)[None, :, None]
    col_ids = jnp.arange(2 * WINDOW, dtype=jnp.int32)[None, None, :]
    offset = row_ids - col_ids + WINDOW
    inside = (offset >= 0) & (offset < WINDOW) & (block_ids * WINDOW - WINDOW + col_ids >= 0)
    weights = softmax_bf16(scores, inside[:, None, None])
    attended = jnp.einsum("bphqk,bkphd->bqphd", weights, v_pair, preferred_element_type=jnp.float32)
    return attended.astype(jnp.bfloat16).reshape(all_frames, positions, heads, width)


def local(
    frame_sequence_elements,
    entry_rescaling_factors,
    asking_projection_tensor,
    lookup_projection_tensor,
    content_projection_tensor,
    logit_sharpness,
    final_projection_tensor,
):
    frames_dev, seq_len, width = frame_sequence_elements.shape
    floated = frame_sequence_elements.astype(jnp.float32)
    rescaled_token_vectors = (
        quadratic_average_rescaling(floated) * entry_rescaling_factors
    ).astype(jnp.bfloat16)
    position_rows = lax.all_to_all(
        rescaled_token_vectors, "frame", split_axis=1, concat_axis=0, tiled=True
    )
    asking_token_vectors, key_matrix_rows, value_matrix_rows = project_through(
        position_rows,
        asking_projection_tensor,
        lookup_projection_tensor,
        content_projection_tensor,
        logit_sharpness,
    )
    result = band_attention(asking_token_vectors, key_matrix_rows, value_matrix_rows)
    attended = lax.all_to_all(result, "frame", split_axis=0, concat_axis=1, tiled=True)
    flat_attended = attended.reshape(frames_dev * seq_len, -1)
    summed = jnp.dot(
        flat_attended, final_projection_tensor, preferred_element_type=jnp.float32
    ) + floated.reshape(frames_dev * seq_len, width)
    return summed.astype(jnp.bfloat16).reshape(frames_dev, seq_len, width)


MESH = pl.DeviceIdType.MESH
HIGH = HEADS_WIN * CHANNELS_PER_ATT


def visiting_order(pairs):
    return sorted(range(1, pairs), key=lambda k: (-abs(k - pairs // 2), k))


def runs(slots):
    found, first = [], 0
    for i in range(1, len(slots) + 1):
        if i == len(slots) or slots[i] != slots[i - 1] + 1:
            found.append((first, i, slots[first]))
            first = i
    return found


def fused(
    devices,
    local_frames,
    sharp_ref,
    x_hbm,
    gain_ref,
    wq_hbm,
    wk_hbm,
    wv_hbm,
    wo_hbm,
    out_ref,
    x_own,
    wq,
    wk,
    wv,
    wo,
    gathered,
    q_rows,
    k_rows,
    v_rows,
    outgoing,
    returned,
    load_sem,
    send_a,
    recv_a,
    send_b,
    recv_b,
):
    me = lax.axis_index("frame")
    block, width = x_own.shape[1], x_own.shape[2]
    positions = block // local_frames
    pairs = devices // 2
    pair, side = me // 2, lax.rem(me, 2)
    partner = me + 1 - 2 * side
    order = visiting_order(pairs)

    barrier = pltpu.get_barrier_semaphore()
    for k in range(1, devices):
        pl.semaphore_signal(
            barrier, inc=1, device_id={"frame": lax.rem(me + k, devices)}, device_id_type=MESH
        )
    loads = [
        pltpu.make_async_copy(source, target, load_sem.at[i])
        for i, (source, target) in enumerate(
            ((x_hbm, x_own), (wq_hbm, wq), (wk_hbm, wk), (wv_hbm, wv), (wo_hbm, wo))
        )
    ]
    for load in loads:
        load.start()
    loads[0].wait()
    pl.semaphore_wait(barrier, devices - 1)

    def send_tokens(target, slot_here, slot_there):
        copy = pltpu.make_async_remote_copy(
            src_ref=x_own.at[target],
            dst_ref=gathered.at[slot_there],
            send_sem=send_a.at[slot_here],
            recv_sem=recv_a.at[slot_there],
            device_id={"frame": target},
            device_id_type=MESH,
        )
        copy.start()
        return copy

    def token_arrival(slot):
        return pltpu.make_async_remote_copy(
            src_ref=x_own.at[0],
            dst_ref=gathered.at[slot],
            send_sem=send_a.at[slot],
            recv_sem=recv_a.at[slot],
            device_id={"frame": partner},
            device_id_type=MESH,
        )

    sent = [send_tokens(partner, 0, side * pairs)]
    for s in range(2):
        for k in order:
            target = lax.rem(pair + k, pairs) * 2 + s
            sent.append(send_tokens(target, s * pairs + k, side * pairs + k))
    gathered[side * pairs] = x_own[me]
    for load in loads[1:]:
        load.wait()

    def project(slots):
        parts = [gathered[slot].astype(jnp.float32) for slot in slots]
        x = jnp.concatenate(parts, axis=0)
        normed = (quadratic_average_rescaling(x) * gain_ref[...].reshape(1, width)).astype(
            jnp.bfloat16
        )
        q = jnp.dot(normed, wq[...], preferred_element_type=jnp.float32)
        k = jnp.dot(normed, wk[...], preferred_element_type=jnp.float32)
        v = jnp.dot(normed, wv[...], preferred_element_type=jnp.float32)
        for h in range(HEADS_WIN):
            c = slice(h * CHANNELS_PER_ATT, (h + 1) * CHANNELS_PER_ATT)
            qs = (
                quadratic_average_rescaling(q[:, c]) * sharp_ref[h] / math.sqrt(CHANNELS_PER_ATT)
            ).astype(jnp.bfloat16)
            ks = quadratic_average_rescaling(k[:, c]).astype(jnp.bfloat16)
            vs = v[:, c].astype(jnp.bfloat16)
            for first, last, to in runs(slots):
                a = slice(first * block, last * block)
                b = slice(to * block, (to + last - first) * block)
                q_rows[b, c] = qs[a]
                k_rows[b, c] = ks[a]
                v_rows[b, c] = vs[a]

    half = pairs // 2
    early, late = [0] + order[: half - 1], order[half - 1 :]
    for piece in (early, late):
        for s in range(2):
            for k in piece:
                if k:
                    token_arrival(s * pairs + k).wait_recv()
        if 0 in piece:
            token_arrival((1 - side) * pairs).wait_recv()
        project(sorted(s * pairs + k for s in range(2) for k in piece))

    total = devices * block
    def ids(axis):
        r = lax.broadcasted_iota(jnp.int32, (total, total), axis)
        slot = r // block
        slot_side = slot // pairs
        source = pair - (slot - slot_side * pairs)
        source = jnp.where(source < 0, source + pairs, source)
        owner = source * 2 + slot_side
        inner = r - slot * block
        return owner * local_frames + inner // positions, inner % positions

    t_row, p_row = ids(0)
    t_col, p_col = ids(1)
    offset = t_row - t_col
    inside = (p_row == p_col) & (offset >= 0) & (offset < WINDOW)
    for h in range(HEADS_WIN):
        c = slice(h * CHANNELS_PER_ATT, (h + 1) * CHANNELS_PER_ATT)
        scores = lax.dot_general(
            q_rows[:, c], k_rows[:, c], (((1,), (1,)), ((), ())), preferred_element_type=jnp.float32
        )
        weights = softmax_bf16(scores, inside)
        attended = jnp.dot(weights, v_rows[:, c], preferred_element_type=jnp.float32)
        outgoing[:, :, c] = attended.reshape(devices, block, CHANNELS_PER_ATT).astype(jnp.bfloat16)

    def send_back(target, slot_here, slot_there):
        copy = pltpu.make_async_remote_copy(
            src_ref=outgoing.at[slot_here],
            dst_ref=returned.at[side, pair],
            send_sem=send_b.at[slot_here],
            recv_sem=recv_b.at[slot_there],
            device_id={"frame": target},
            device_id_type=MESH,
        )
        copy.start()
        return copy

    def arrival(s, k):
        return pltpu.make_async_remote_copy(
            src_ref=outgoing.at[0],
            dst_ref=returned.at[s, lax.rem(pair + k, pairs)],
            send_sem=send_b.at[0],
            recv_sem=recv_b.at[s * pairs + k],
            device_id={"frame": partner},
            device_id_type=MESH,
        )

    for k in order:
        for s in range(2):
            target = lax.rem(pair + pairs - k, pairs) * 2 + s
            sent.append(send_back(target, s * pairs + k, side * pairs + k))
    sent.append(send_back(partner, (1 - side) * pairs, side * pairs))
    returned[side, pair] = outgoing[side * pairs]
    arrival(1 - side, 0).wait_recv()
    for s in range(2):
        for k in order:
            arrival(s, k).wait_recv()
        rows = pairs * block
        mixed = returned[s].astype(jnp.float32).reshape(rows, HIGH).astype(jnp.bfloat16)
        summed = jnp.dot(mixed, wo[...], preferred_element_type=jnp.float32)
        for k in range(pairs):
            j = 2 * k + s
            out_ref[j] = (
                summed[k * block : (k + 1) * block] + x_own[j].astype(jnp.float32)
            ).astype(jnp.bfloat16)
    for copy in sent:
        copy.wait_send()


def local_fused(devices, x, gain, wq, wk, wv, sharp, wo):
    local_frames, seq_len, width = x.shape
    positions = seq_len // devices
    block = local_frames * positions
    total = devices * block
    blocks = x.reshape(local_frames, devices, positions, width)
    blocks = blocks.transpose(1, 0, 2, 3).reshape(devices, block, width)
    vmem = pl.BlockSpec(memory_space=pltpu.VMEM)
    anywhere = pl.BlockSpec(memory_space=pl.ANY)
    dma = pltpu.SemaphoreType.DMA
    out = pl.pallas_call(
        functools.partial(fused, devices, local_frames),
        out_shape=pltpu.VMEM(blocks.shape, jnp.bfloat16),
        in_specs=[pl.BlockSpec(memory_space=pltpu.SMEM), anywhere, vmem] + [anywhere] * 4,
        out_specs=vmem,
        scratch_shapes=[
            pltpu.VMEM(blocks.shape, jnp.bfloat16),
            pltpu.VMEM(wq.shape, jnp.bfloat16),
            pltpu.VMEM(wk.shape, jnp.bfloat16),
            pltpu.VMEM(wv.shape, jnp.bfloat16),
            pltpu.VMEM(wo.shape, jnp.bfloat16),
            pltpu.VMEM(blocks.shape, jnp.bfloat16),
            pltpu.VMEM((total, HIGH), jnp.bfloat16),
            pltpu.VMEM((total, HIGH), jnp.bfloat16),
            pltpu.VMEM((total, HIGH), jnp.bfloat16),
            pltpu.VMEM((devices, block, HIGH), jnp.bfloat16),
            pltpu.VMEM((2, devices // 2, block, HIGH), jnp.bfloat16),
            dma((5,)),
            dma((devices,)),
            dma((devices,)),
            dma((devices,)),
            dma((devices,)),
        ],
        compiler_params=pltpu.CompilerParams(
            collective_id=0, has_side_effects=True, vmem_limit_bytes=60 * 2**20
        ),
    )(sharp, blocks, gain, wq, wk, wv, wo)
    out = out.reshape(devices, local_frames, positions, width).transpose(1, 0, 2, 3)
    return out.reshape(x.shape)


def solution(mesh):
    devices = mesh.shape["frame"]

    def body(x, *rest):
        positions = x.shape[1] // devices
        if devices % 4 == 0 and positions % 8 == 0:
            return local_fused(devices, x, *rest)
        return local(x, *rest)

    placed = (P(("clips", "frame"), None, None), P(), P(), P(), P(), P(), P())
    return jax.shard_map(
        body,
        mesh=mesh,
        in_specs=placed,
        out_specs=P(("clips", "frame"), None, None),
        check_vma=False,
    )
```

```python
import functools
import math

import jax
import jax.numpy as jnp
from jax import lax
from jax.experimental import pallas as pl
from jax.experimental.pallas import tpu as pltpu
from jax.sharding import PartitionSpec as P

HEADS_WIN = 5
CHANNELS_PER_ATT = 128
WINDOW = 32


epsilon = 1e-06


def quadratic_average_rescaling(values):
    return values * lax.rsqrt(jnp.mean(values * values, axis=-1, keepdims=True) + epsilon)


def project_through(
    incoming_token_vectors,
    asking_projection_tensor,
    lookup_projection_tensor,
    content_projection_tensor,
    logit_sharpness,
):
    lead = incoming_token_vectors.shape[:-1]
    flat_rows = incoming_token_vectors.reshape(-1, incoming_token_vectors.shape[-1])
    shape_heads = lead + (HEADS_WIN, CHANNELS_PER_ATT)
    asking_vectors_full = jnp.dot(
        flat_rows, asking_projection_tensor, preferred_element_type=jnp.float32
    ).reshape(shape_heads)
    k_full = jnp.dot(
        flat_rows, lookup_projection_tensor, preferred_element_type=jnp.float32
    ).reshape(shape_heads)
    v_full = jnp.dot(
        flat_rows, content_projection_tensor, preferred_element_type=jnp.float32
    ).reshape(shape_heads)
    asking_token_vectors = (
        quadratic_average_rescaling(asking_vectors_full)
        * logit_sharpness[:, None]
        / math.sqrt(CHANNELS_PER_ATT)
    ).astype(jnp.bfloat16)
    key_matrix_rows = quadratic_average_rescaling(k_full).astype(jnp.bfloat16)
    return (asking_token_vectors, key_matrix_rows, v_full.astype(jnp.bfloat16))


def softmax_bf16(scores, window_mask):
    scores = jnp.where(window_mask, scores, -1e30)
    top = jnp.max(scores, axis=-1, keepdims=True)
    expo = jnp.exp(scores - top)
    return (expo / jnp.sum(expo, axis=-1, keepdims=True)).astype(jnp.bfloat16)


def band_attention(asking_token_vectors, key_matrix_rows, value_matrix_rows):
    all_frames, positions, heads, width = asking_token_vectors.shape
    blocks = all_frames // WINDOW
    block_shape = (blocks, WINDOW, positions, heads, width)
    q_blocks = asking_token_vectors.reshape(block_shape)
    k_blocks = key_matrix_rows.reshape(block_shape)
    v_blocks = value_matrix_rows.reshape(block_shape)
    k_earlier = jnp.concatenate([jnp.zeros_like(k_blocks[:1]), k_blocks[:-1]], axis=0)
    v_earlier = jnp.concatenate([jnp.zeros_like(v_blocks[:1]), v_blocks[:-1]], axis=0)
    k_pair = jnp.concatenate([k_earlier, k_blocks], axis=1)
    v_pair = jnp.concatenate([v_earlier, v_blocks], axis=1)
    scores = jnp.einsum("bqphd,bkphd->bphqk", q_blocks, k_pair, preferred_element_type=jnp.float32)
    block_ids = jnp.arange(blocks, dtype=jnp.int32)[:, None, None]
    row_ids = jnp.arange(WINDOW, dtype=jnp.int32)[None, :, None]
    col_ids = jnp.arange(2 * WINDOW, dtype=jnp.int32)[None, None, :]
    offset = row_ids - col_ids + WINDOW
    inside = (offset >= 0) & (offset < WINDOW) & (block_ids * WINDOW - WINDOW + col_ids >= 0)
    weights = softmax_bf16(scores, inside[:, None, None])
    attended = jnp.einsum("bphqk,bkphd->bqphd", weights, v_pair, preferred_element_type=jnp.float32)
    return attended.astype(jnp.bfloat16).reshape(all_frames, positions, heads, width)


def local(
    frame_sequence_elements,
    entry_rescaling_factors,
    asking_projection_tensor,
    lookup_projection_tensor,
    content_projection_tensor,
    logit_sharpness,
    final_projection_tensor,
):
    frames_dev, seq_len, width = frame_sequence_elements.shape
    floated = frame_sequence_elements.astype(jnp.float32)
    rescaled_token_vectors = (
        quadratic_average_rescaling(floated) * entry_rescaling_factors
    ).astype(jnp.bfloat16)
    position_rows = lax.all_to_all(
        rescaled_token_vectors, "frame", split_axis=1, concat_axis=0, tiled=True
    )
    asking_token_vectors, key_matrix_rows, value_matrix_rows = project_through(
        position_rows,
        asking_projection_tensor,
        lookup_projection_tensor,
        content_projection_tensor,
        logit_sharpness,
    )
    result = band_attention(asking_token_vectors, key_matrix_rows, value_matrix_rows)
    attended = lax.all_to_all(result, "frame", split_axis=0, concat_axis=1, tiled=True)
    flat_attended = attended.reshape(frames_dev * seq_len, -1)
    summed = jnp.dot(
        flat_attended, final_projection_tensor, preferred_element_type=jnp.float32
    ) + floated.reshape(frames_dev * seq_len, width)
    return summed.astype(jnp.bfloat16).reshape(frames_dev, seq_len, width)


MESH = pl.DeviceIdType.MESH
HIGH = HEADS_WIN * CHANNELS_PER_ATT


def visiting_order(pairs):
    return sorted(range(1, pairs), key=lambda k: (-abs(k - pairs // 2), k))


def runs(slots):
    found, first = [], 0
    for i in range(1, len(slots) + 1):
        if i == len(slots) or slots[i] != slots[i - 1] + 1:
            found.append((first, i, slots[first]))
            first = i
    return found


def fused(
    devices,
    local_frames,
    sharp_ref,
    x_hbm,
    gain_ref,
    wq_hbm,
    wk_hbm,
    wv_hbm,
    wo_hbm,
    out_ref,
    x_own,
    wq,
    wk,
    wv,
    wo,
    gathered,
    q_rows,
    k_rows,
    v_rows,
    outgoing,
    returned,
    load_sem,
    send_a,
    recv_a,
    send_b,
    recv_b,
):
    me = lax.axis_index("frame")
    block, width = x_own.shape[1], x_own.shape[2]
    positions = block // local_frames
    pairs = devices // 2
    pair, side = me // 2, lax.rem(me, 2)
    partner = me + 1 - 2 * side
    order = visiting_order(pairs)

    barrier = pltpu.get_barrier_semaphore()
    for k in range(1, devices):
        pl.semaphore_signal(
            barrier, inc=1, device_id={"frame": lax.rem(me + k, devices)}, device_id_type=MESH
        )
    loads = [
        pltpu.make_async_copy(source, target, load_sem.at[i])
        for i, (source, target) in enumerate(
            ((x_hbm, x_own), (wq_hbm, wq), (wk_hbm, wk), (wv_hbm, wv), (wo_hbm, wo))
        )
    ]
    for load in loads:
        load.start()
    loads[0].wait()
    pl.semaphore_wait(barrier, devices - 1)

    def send_tokens(target, slot_here, slot_there):
        copy = pltpu.make_async_remote_copy(
            src_ref=x_own.at[target],
            dst_ref=gathered.at[slot_there],
            send_sem=send_a.at[slot_here],
            recv_sem=recv_a.at[slot_there],
            device_id={"frame": target},
            device_id_type=MESH,
        )
        copy.start()
        return copy

    def token_arrival(slot):
        return pltpu.make_async_remote_copy(
            src_ref=x_own.at[0],
            dst_ref=gathered.at[slot],
            send_sem=send_a.at[slot],
            recv_sem=recv_a.at[slot],
            device_id={"frame": partner},
            device_id_type=MESH,
        )

    sent = [send_tokens(partner, 0, side * pairs)]
    for s in range(2):
        for k in order:
            target = lax.rem(pair + k, pairs) * 2 + s
            sent.append(send_tokens(target, s * pairs + k, side * pairs + k))
    gathered[side * pairs] = x_own[me]
    for load in loads[1:]:
        load.wait()

    def project(slots):
        parts = [gathered[slot].astype(jnp.float32) for slot in slots]
        x = jnp.concatenate(parts, axis=0)
        normed = (quadratic_average_rescaling(x) * gain_ref[...].reshape(1, width)).astype(
            jnp.bfloat16
        )
        q = jnp.dot(normed, wq[...], preferred_element_type=jnp.float32)
        k = jnp.dot(normed, wk[...], preferred_element_type=jnp.float32)
        v = jnp.dot(normed, wv[...], preferred_element_type=jnp.float32)
        for h in range(HEADS_WIN):
            c = slice(h * CHANNELS_PER_ATT, (h + 1) * CHANNELS_PER_ATT)
            qs = (
                quadratic_average_rescaling(q[:, c]) * sharp_ref[h] / math.sqrt(CHANNELS_PER_ATT)
            ).astype(jnp.bfloat16)
            ks = quadratic_average_rescaling(k[:, c]).astype(jnp.bfloat16)
            vs = v[:, c].astype(jnp.bfloat16)
            for first, last, to in runs(slots):
                a = slice(first * block, last * block)
                b = slice(to * block, (to + last - first) * block)
                q_rows[b, c] = qs[a]
                k_rows[b, c] = ks[a]
                v_rows[b, c] = vs[a]

    total = devices * block

    def ids(axis):
        shape = (total, 1) if axis == 0 else (1, total)
        r = lax.broadcasted_iota(jnp.int32, shape, axis)
        slot = r // block
        slot_side = slot // pairs
        source = pair - (slot - slot_side * pairs)
        source = jnp.where(source < 0, source + pairs, source)
        owner = source * 2 + slot_side
        inner = r - slot * block
        return owner * local_frames + inner // positions, inner % positions

    t_row, p_row = ids(0)
    t_col, p_col = ids(1)
    offset = t_row - t_col
    inside = (p_row == p_col) & (offset >= 0) & (offset < WINDOW)
    half = pairs // 2
    early, late = [0] + order[: half - 1], order[half - 1 :]
    for piece in (early, late):
        for s in range(2):
            for k in piece:
                if k:
                    token_arrival(s * pairs + k).wait_recv()
        if 0 in piece:
            token_arrival((1 - side) * pairs).wait_recv()
        project(sorted(s * pairs + k for s in range(2) for k in piece))

    for h in range(HEADS_WIN):
        c = slice(h * CHANNELS_PER_ATT, (h + 1) * CHANNELS_PER_ATT)
        scores = lax.dot_general(
            q_rows[:, c], k_rows[:, c], (((1,), (1,)), ((), ())), preferred_element_type=jnp.float32
        )
        weights = softmax_bf16(scores, inside)
        attended = jnp.dot(weights, v_rows[:, c], preferred_element_type=jnp.float32)
        outgoing[:, :, c] = attended.reshape(devices, block, CHANNELS_PER_ATT).astype(jnp.bfloat16)

    def send_back(target, slot_here, slot_there):
        copy = pltpu.make_async_remote_copy(
            src_ref=outgoing.at[slot_here],
            dst_ref=returned.at[side, pair],
            send_sem=send_b.at[slot_here],
            recv_sem=recv_b.at[slot_there],
            device_id={"frame": target},
            device_id_type=MESH,
        )
        copy.start()
        return copy

    def arrival(s, k):
        return pltpu.make_async_remote_copy(
            src_ref=outgoing.at[0],
            dst_ref=returned.at[s, lax.rem(pair + k, pairs)],
            send_sem=send_b.at[0],
            recv_sem=recv_b.at[s * pairs + k],
            device_id={"frame": partner},
            device_id_type=MESH,
        )

    for k in order:
        for s in range(2):
            target = lax.rem(pair + pairs - k, pairs) * 2 + s
            sent.append(send_back(target, s * pairs + k, side * pairs + k))
    sent.append(send_back(partner, (1 - side) * pairs, side * pairs))
    returned[side, pair] = outgoing[side * pairs]
    arrival(1 - side, 0).wait_recv()
    for s in range(2):
        for k in order:
            arrival(s, k).wait_recv()
        rows = pairs * block
        mixed = returned[s].astype(jnp.float32).reshape(rows, HIGH).astype(jnp.bfloat16)
        summed = jnp.dot(mixed, wo[...], preferred_element_type=jnp.float32)
        for k in range(pairs):
            j = 2 * k + s
            out_ref[j] = (
                summed[k * block : (k + 1) * block] + x_own[j].astype(jnp.float32)
            ).astype(jnp.bfloat16)
    for copy in sent:
        copy.wait_send()


def local_fused(devices, x, gain, wq, wk, wv, sharp, wo):
    local_frames, seq_len, width = x.shape
    positions = seq_len // devices
    block = local_frames * positions
    total = devices * block
    blocks = x.reshape(local_frames, devices, positions, width)
    blocks = blocks.transpose(1, 0, 2, 3).reshape(devices, block, width)
    vmem = pl.BlockSpec(memory_space=pltpu.VMEM)
    anywhere = pl.BlockSpec(memory_space=pl.ANY)
    dma = pltpu.SemaphoreType.DMA
    out = pl.pallas_call(
        functools.partial(fused, devices, local_frames),
        out_shape=pltpu.VMEM(blocks.shape, jnp.bfloat16),
        in_specs=[pl.BlockSpec(memory_space=pltpu.SMEM), anywhere, vmem] + [anywhere] * 4,
        out_specs=vmem,
        scratch_shapes=[
            pltpu.VMEM(blocks.shape, jnp.bfloat16),
            pltpu.VMEM(wq.shape, jnp.bfloat16),
            pltpu.VMEM(wk.shape, jnp.bfloat16),
            pltpu.VMEM(wv.shape, jnp.bfloat16),
            pltpu.VMEM(wo.shape, jnp.bfloat16),
            pltpu.VMEM(blocks.shape, jnp.bfloat16),
            pltpu.VMEM((total, HIGH), jnp.bfloat16),
            pltpu.VMEM((total, HIGH), jnp.bfloat16),
            pltpu.VMEM((total, HIGH), jnp.bfloat16),
            pltpu.VMEM((devices, block, HIGH), jnp.bfloat16),
            pltpu.VMEM((2, devices // 2, block, HIGH), jnp.bfloat16),
            dma((5,)),
            dma((devices,)),
            dma((devices,)),
            dma((devices,)),
            dma((devices,)),
        ],
        compiler_params=pltpu.CompilerParams(
            collective_id=0, has_side_effects=True, vmem_limit_bytes=60 * 2**20
        ),
    )(sharp, blocks, gain, wq, wk, wv, wo)
    out = out.reshape(devices, local_frames, positions, width).transpose(1, 0, 2, 3)
    return out.reshape(x.shape)


def solution(mesh):
    devices = mesh.shape["frame"]

    def body(x, *rest):
        positions = x.shape[1] // devices
        if devices % 4 == 0 and positions % 8 == 0:
            return local_fused(devices, x, *rest)
        return local(x, *rest)

    placed = (P(("clips", "frame"), None, None), P(), P(), P(), P(), P(), P())
    return jax.shard_map(
        body,
        mesh=mesh,
        in_specs=placed,
        out_specs=P(("clips", "frame"), None, None),
        check_vma=False,
    )
```
